32 devices in a mesh: gx: 4 (over y, x), gy: 4 (over z), gz: 2 (over core).
Axes of the slice: x: 2, y: 2, z: 4, core: 2. Of those that a mesh axis runs over, the one named last changes fastest.
Arguments:
- right_side: float32 [5, 512, 8, 128], P(None, ('gx', 'gy', 'gz')), may hold values from -6 to 6
- diag_inverse: bfloat16 [5, 512, 128, 128], P(None, ('gx', 'gy', 'gz')), may hold values from -0.5 to 0.5
- off_blocks: bfloat16 [4, 1024, 128, 128], P(None, ('gx', 'gy', 'gz')), may hold values from -0.375 to 0.375
- live_counts: int32 [5, 32], P(None, ('gx', 'gy', 'gz')), may hold values from 1 to 16, as said below
- source_slot: int32 [4, 1024], P(None, ('gx', 'gy', 'gz')), may hold values from 0 to 15, as said below
- target_owner: int32 [4, 1024], P(None, ('gx', 'gy', 'gz')), may hold values from 0 to 31, as said below
- target_block: int32 [4, 1024], P(None, ('gx', 'gy', 'gz')), may hold values from 16 to 79, as said below
Outputs:
- solution: float32 [5, 512, 8, 128], P(None, ('gx', 'gy', 'gz'))
The draws below stay inside these ranges and needn't reach their ends.
Inputs may be any that keep to these rules, and one draw needn't show every extreme that they name: `live_counts`: slots at or past a device's count in a level are empty; in every level some device has all 16 slots live. `source_slot`: names a live slot of the issuing device in the same level. `target_owner`: in every level, each device's records go exactly 2 each to 16 distinct owners and none to the others. `target_block`: the level part is later than the record's own level, and the slot is live at the owner in that level.
All inputs are finite; a program needn't handle non-finite values.
Results may differ from the reference program's by a relative error of at most 0.013.
Values sent between devices are 32-bit elements; how exact they have to be, the bound alone decides.
No kernel may reach another device: no remote copies, remote signals or barrier semaphores. Data moves between devices by JAX's collectives and lax.ppermute only.
A program may use at most 64 MiB of HBM per device.

```python
import jax
import jax.numpy as jnp
from jax import lax

B = 128
R = 8
LEVELS = 5
S = 16
CAP = 2
OWNERS = 32
RECS = 32
NBLK = 512


def routing(key):
    base = jax.random.fold_in(key, 7)
    key_count, key_full, key_perm, key_src, key_level, key_slot = jax.random.split(base, 6)
    counts = jax.random.randint(key_count, (LEVELS, OWNERS), 1, S + 1)
    full_owner = jax.random.randint(key_full, (LEVELS,), 0, OWNERS)
    counts = counts.at[jnp.arange(LEVELS), full_owner].set(S)

    def one_list(sub_key):
        first_key, second_key = jax.random.split(sub_key)
        chosen = jax.random.permutation(first_key, OWNERS)[:OWNERS // 2].astype(jnp.int32)
        whole_list = jnp.repeat(chosen, CAP)
        return whole_list[jax.random.permutation(second_key, RECS)]
    list_keys = jax.random.split(key_perm, (LEVELS - 1) * OWNERS)
    owners = jax.vmap(one_list)(list_keys).reshape(LEVELS - 1, OWNERS, RECS)
    shape = (LEVELS - 1, OWNERS, RECS)
    sources = jax.random.randint(key_src, shape, 0, counts[:-1, :, None])
    lowest = (jnp.arange(LEVELS - 1, dtype=jnp.int32) + 1)[:, None, None]
    target_level = jax.random.randint(key_level, shape, lowest, LEVELS)
    target_slot = jax.random.randint(key_slot, shape, 0, counts[target_level, owners])
    blocks = target_level * S + target_slot
    flat = (LEVELS - 1, OWNERS * RECS)
    return (counts.astype(jnp.int32), sources.reshape(flat).astype(jnp.int32), owners.reshape(flat).astype(jnp.int32), blocks.reshape(flat).astype(jnp.int32))


def draw_live_counts(key, part):
    return routing(key)[0]


def draw_source_slot(key, part):
    return routing(key)[1]


def draw_target_owner(key, part):
    return routing(key)[2]


def draw_target_block(key, part):
    return routing(key)[3]


def block_scale(stream_key, shape, cuts, low, high):
    def one(position, shards_of):
        steps = jax.random.uniform(jax.random.fold_in(jax.random.fold_in(stream_key, 6), position), (shards_of,), jnp.float32, low / len(cuts), high / len(cuts))
        return jnp.repeat(jnp.exp(steps), shape[position] // shards_of).reshape((-1,) + (1,) * (len(shape) - position - 1))

    gain = one(*cuts[0])
    for cut in cuts[1:]:
        gain = gain * one(*cut)
    return gain


def scatter_about(own_key, shape, scale, bound, cuts=(), kind=jnp.bfloat16):
    drawn = scale * jax.random.normal(own_key, shape, jnp.float32)
    if cuts:
        drawn = drawn * block_scale(own_key, shape, cuts, -0.22, 0.18)
    return jnp.clip(drawn, -bound, bound).astype(kind)


def setup_inputs(seed: int = 0) -> dict:
    streams_of = jax.random.split(jax.random.key(seed), 8)
    right_side = scatter_about(streams_of[0], (LEVELS, NBLK, R, B), 1.0, 6.0, ((1, 32),), jnp.float32)
    diag_inverse = scatter_about(streams_of[1], (LEVELS, NBLK, B, B), B ** -0.5, 0.5, ((1, 32),))
    off_blocks = scatter_about(streams_of[2], (LEVELS - 1, OWNERS * RECS, B, B), (2 * B) ** -0.5, 0.375, ((1, 32),))
    live_counts = draw_live_counts(jax.random.fold_in(streams_of[7], 71), 0)
    source_slot = draw_source_slot(jax.random.fold_in(streams_of[7], 71), 0)
    target_owner = draw_target_owner(jax.random.fold_in(streams_of[7], 71), 0)
    target_block = draw_target_block(jax.random.fold_in(streams_of[7], 71), 0)
    return {"right_side": right_side, "diag_inverse": diag_inverse, "off_blocks": off_blocks, "live_counts": live_counts, "source_slot": source_slot, "target_owner": target_owner, "target_block": target_block}


def reference(right_side, diag_inverse, off_blocks, live_counts, source_slot, target_owner, target_block):
    accumulated = jnp.zeros((LEVELS * NBLK, R, B), jnp.float32)
    slot_ids = jnp.arange(S, dtype=jnp.int32)
    solved_all = []
    for level_at in range(LEVELS):
        live = (slot_ids[None, :] < live_counts[level_at][:, None]).reshape(NBLK)
        pending = accumulated[level_at * NBLK:(level_at + 1) * NBLK]
        work_rows = (right_side[level_at] - pending).astype(jnp.bfloat16)
        solved = jnp.einsum('nrb,nbc->nrc', work_rows.astype(jnp.float32), diag_inverse[level_at].astype(jnp.float32))
        solved = jnp.where(live[:, None, None], solved, jnp.float32(0.0))
        solved_all.append(solved)
        if level_at + 1 < LEVELS:
            rounded = solved.astype(jnp.bfloat16).reshape(OWNERS, S, R, B)
            blocks = off_blocks[level_at].reshape(OWNERS, RECS, B, B)
            slot_lists = source_slot[level_at].reshape(OWNERS, RECS)

            def per_owner(items):
                owner_rows, owner_blocks, owner_slots = items
                picked = owner_rows[owner_slots]
                return jnp.einsum('krb,kbc->krc', picked.astype(jnp.float32), owner_blocks.astype(jnp.float32))

            contributions = lax.map(per_owner, (rounded, blocks, slot_lists)).reshape(OWNERS * RECS, R, B)
            owner_ids = target_owner[level_at].astype(jnp.int32)
            targets = target_block[level_at].astype(jnp.int32)
            row_ids = (targets // S) * NBLK + owner_ids * S + targets % S
            accumulated = accumulated.at[row_ids].add(contributions)
    return jnp.stack(solved_all)
```

```python
import functools

import jax
import jax.numpy as jnp
from jax import lax
from jax.experimental import pallas as pl
from jax.experimental.pallas import tpu as pltpu
from jax.sharding import PartitionSpec as P


CAP = 2
AXES = ("gx", "gy", "gz")
VMEM = pl.BlockSpec(memory_space=pltpu.VMEM)
SMEM = pl.BlockSpec(memory_space=pltpu.SMEM)
HBM = pl.BlockSpec(memory_space=pltpu.HBM)
PARAMS = pltpu.CompilerParams(vmem_limit_bytes=16 * 1024 * 1024)


def assign_places(target, taken, owners, store):
    for level in range(target.shape[0]):
        for owner in range(owners):
            taken[owner] = 0
        for record in range(target.shape[1]):
            owner = target[level, record]
            count = taken[owner]
            taken[owner] = count + 1
            store(level, record, owner * CAP + count)


def solve(live_count, work_of, diag, solved):
    for slot in range(solved.shape[0]):
        work = work_of(slot).astype(jnp.bfloat16)
        out = jnp.dot(work, diag[slot], preferred_element_type=jnp.float32)
        solved[slot] = jnp.where(slot < live_count, out, jnp.zeros_like(out))


def first_kernel(owners, slots, *refs):
    live, source, target, owner_rows, block_rows, rhs, diag, off = refs[:8]
    answer, outgoing, token, rhs_now, diag_now, off_now, solved, taken, place, sems = refs[8:]
    load_rhs = pltpu.make_async_copy(rhs.at[0], rhs_now, sems.at[0])
    load_diag = pltpu.make_async_copy(diag.at[0], diag_now, sems.at[1])
    load_off = pltpu.make_async_copy(off.at[0], off_now, sems.at[2])
    load_rhs.start()
    load_diag.start()
    load_off.start()
    token[0] = 0
    steps, records = owner_rows.shape
    rows, width = solved.shape[1:]
    chunk = CAP * rows + 1
    out = outgoing.reshape(owners * chunk, width)

    def keep(level, record, where):
        place[record] = (where // CAP) * chunk + (where % CAP) * rows

    assign_places(target.at[pl.ds(0, 1)], taken, owners, keep)
    blocks = (steps + 1) * slots
    base = 1 << blocks.bit_length()
    none = jnp.float32(records * base)
    ids = lax.broadcasted_iota(jnp.int32, (owners, records), 0)
    order = lax.broadcasted_iota(jnp.int32, (owners, records), 1) * base
    lane = lax.broadcasted_iota(jnp.int32, (owners, width), 1)
    labels = jnp.zeros((owners, width), jnp.float32)
    for level in range(steps):
        hit = owner_rows[level : level + 1, :] == ids
        coded = (order + block_rows[level : level + 1, :]).astype(jnp.float32)
        low = jnp.min(jnp.where(hit, coded, none), axis=1, keepdims=True)
        high = jnp.max(jnp.where(hit, coded, jnp.float32(-1)), axis=1, keepdims=True)
        for at, value in enumerate((low, high)):
            label = (value.astype(jnp.int32) & (base - 1)).astype(jnp.float32)
            label = jnp.where(low < none, label, jnp.float32(blocks))
            labels = jnp.where(lane == level * CAP + at, label, labels)
    for owner in range(owners):
        out[owner * chunk + CAP * rows : (owner + 1) * chunk, :] = labels[owner : owner + 1, :]
    load_rhs.wait()
    load_diag.wait()
    solve(live[0], lambda slot: rhs_now[slot], diag_now, solved)
    store = pltpu.make_async_copy(solved, answer.at[0], sems.at[3])
    store.start()
    load_off.wait()
    for record in range(records):
        picked = solved[source[0, record]].astype(jnp.bfloat16)
        value = jnp.dot(picked, off_now[record], preferred_element_type=jnp.float32)
        out[pl.ds(place[record], rows), :] = value
    store.wait()


def fetch_kernel(owners, token, live, source, target, rhs, diag, off, *refs):
    live_now, source_now, place_now, rhs_now, diag_now, diag_next, off_now, taken, sems = refs
    loads = (
        (live, live_now),
        (source, source_now),
        (rhs.at[1], rhs_now),
        (diag.at[1], diag_now),
        (off.at[1], off_now),
        (diag.at[2], diag_next),
    )
    copies = [pltpu.make_async_copy(x, y, sems.at[at]) for at, (x, y) in enumerate(loads)]
    for copy in copies:
        copy.start()

    def keep(level, record, where):
        place_now[level, record] = where

    assign_places(target, taken, owners, keep)
    for copy in copies:
        copy.wait()


def later_kernel(level, levels, owners, *refs):
    last = level == levels - 1
    refs = list(refs)
    live, rhs, diag, arrived = refs[:4]
    refs = refs[4:]
    labels = refs.pop(0) if level > 1 else None
    if not last:
        source, place, off = refs[:3]
        refs = refs[3:]
        rhs_all = refs.pop(0)
        diag_all, off_all = (refs.pop(0), refs.pop(0)) if level < levels - 2 else (None, None)
    before = refs.pop(0) if level > 1 else None
    refs.pop(0)
    answer = refs.pop(0)
    if not last:
        outgoing, after, rhs_near = refs[:3]
        refs = refs[3:]
        diag_near, off_near = (refs.pop(0), refs.pop(0)) if diag_all is not None else (None, None)
    if level == 1:
        labels = refs.pop(0)
    solved, total, sems = refs[:3]
    sem = sems.at[0]
    ahead = []
    if not last:
        ahead.append(pltpu.make_async_copy(rhs_all.at[level + 1], rhs_near, sems.at[1]))
        if diag_all is not None:
            ahead.append(pltpu.make_async_copy(off_all.at[level + 1], off_near, sems.at[2]))
            ahead.append(pltpu.make_async_copy(diag_all.at[level + 2], diag_near, sems.at[3]))
    for copy in ahead:
        copy.start()
    slots, rows, width = solved.shape
    left = levels - level
    chunk = CAP * rows
    if level == 1:
        gathered, turned = refs[3:]
        flat = arrived.reshape(arrived.shape[0], width)
        for owner in range(owners):
            at = owner * (chunk + 1) + chunk
            gathered[owner : owner + 1, :] = flat[at : at + 1, :]
        turned[...] = gathered[...].T[: turned.shape[0], :].astype(jnp.int32)
        copy = pltpu.make_async_copy(turned, labels, sem)
        copy.start()
        total[...] = jnp.zeros_like(total)
        copy.wait()
    else:
        total[0 : left * slots] = before[...]
    for owner in range(owners):
        for at in range(CAP):
            label = labels[(level - 1) * CAP + at, owner] - level * slots
            if level == 1:
                start = owner * (chunk + 1) + at * rows
                value = flat[start : start + rows, :]
            else:
                value = arrived[owner * CAP + at]
            total[label] += value
    solve(live[level], lambda slot: rhs[slot] - total[slot], diag, solved)
    store = pltpu.make_async_copy(solved, answer.at[level], sem)
    store.start()
    if not last:
        for record in range(off.shape[0]):
            picked = solved[source[level, record]].astype(jnp.bfloat16)
            value = jnp.dot(picked, off[record], preferred_element_type=jnp.float32)
            outgoing[place[level, record]] = value
        after[...] = total[slots : left * slots]
    store.wait()
    for copy in ahead:
        copy.wait()


def shards(right_side, diag_inverse, off_blocks, live_counts, source_slot, target_owner, target_block):
    levels, slots, rows, width = right_side.shape
    records = off_blocks.shape[1]
    owners = lax.axis_size(AXES)
    steps = levels - 1
    chunk = CAP * rows
    f32, bf16, i32 = jnp.float32, jnp.bfloat16, jnp.int32
    near, table, semaphores = pltpu.VMEM, pltpu.SMEM, pltpu.SemaphoreType.DMA
    in_hbm = functools.partial(pltpu.with_memory_space_constraint, memory_space=pltpu.HBM)
    live, source, target, rhs, diag, off = (
        in_hbm(x)
        for x in (live_counts.reshape(levels), source_slot, target_owner, right_side, diag_inverse, off_blocks)
    )

    def exchange(parts):
        return lax.all_to_all(parts, AXES, split_axis=0, concat_axis=0, tiled=True)

    answer, outgoing, token = pl.pallas_call(
        functools.partial(first_kernel, owners, slots),
        out_shape=[
            pltpu.HBM((levels, slots, rows, width), f32),
            near((owners * (chunk + 1), 1, width), f32),
            table((1,), i32),
        ],
        in_specs=[SMEM] * 3 + [VMEM] * 2 + [HBM] * 3,
        out_specs=[HBM, VMEM, SMEM],
        scratch_shapes=[
            near((slots, rows, width), f32),
            near((slots, width, width), bf16),
            near((records, width, width), bf16),
            near((slots, rows, width), f32),
            table((owners,), i32),
            table((records,), i32),
            semaphores((4,)),
        ],
        name="level_0",
        compiler_params=PARAMS,
    )(live, source, target, target, in_hbm(target_block), rhs, diag, off)
    arrived = exchange(outgoing.reshape(owners, chunk + 1, 1, width))
    arrived = arrived.reshape(owners * (chunk + 1), 1, width)

    live, source, place, rhs_now, diag_now, diag_next, off_now = pl.pallas_call(
        functools.partial(fetch_kernel, owners),
        out_shape=[
            table((levels,), i32),
            table((steps, records), i32),
            table((steps, records), i32),
            near((slots, rows, width), f32),
            near((slots, width, width), bf16),
            near((slots, width, width), bf16),
            near((records, width, width), bf16),
        ],
        in_specs=[SMEM, HBM, HBM, SMEM] + [HBM] * 3,
        out_specs=[SMEM] * 3 + [VMEM] * 4,
        scratch_shapes=[table((owners,), i32), semaphores((6,))],
        name="fetch",
        compiler_params=PARAMS,
    )(token, live, source, target, rhs, diag, off)

    labels = before = None
    for level in range(1, levels):
        last = level == levels - 1
        left = levels - level
        operands = [(live, SMEM), (rhs_now, VMEM), (diag_now, VMEM), (arrived, VMEM)]
        if level > 1:
            operands.append((labels, SMEM))
        if not last:
            operands += [(source, SMEM), (place, SMEM), (off_now, VMEM), (rhs, HBM)]
            if level < steps - 1:
                operands += [(diag, HBM), (off, HBM)]
        if level > 1:
            operands.append((before, VMEM))
        operands.append((in_hbm(answer), HBM))
        outs = [(pltpu.HBM((levels, slots, rows, width), f32), HBM)]
        scratch = [near((slots, rows, width), f32), near((left * slots + 1, rows, width), f32)]
        scratch.append(semaphores((4,)))
        if not last:
            outs.append((near((owners * CAP, rows, width), f32), VMEM))
            outs.append((near(((left - 1) * slots, rows, width), f32), VMEM))
            outs.append((near((slots, rows, width), f32), VMEM))
            if level < steps - 1:
                outs.append((near((slots, width, width), bf16), VMEM))
                outs.append((near((records, width, width), bf16), VMEM))
        if level == 1:
            outs.append((table((steps * CAP, owners), i32), SMEM))
            scratch += [near((owners, width), f32), near((steps * CAP, owners), i32)]
        made = pl.pallas_call(
            functools.partial(later_kernel, level, levels, owners),
            out_shape=[shape for shape, _ in outs],
            in_specs=[spec for _, spec in operands],
            out_specs=[spec for _, spec in outs],
            input_output_aliases={len(operands) - 1: 0},
            scratch_shapes=scratch,
            compiler_params=PARAMS,
        )(*[value for value, _ in operands])
        answer = made[0]
        if last:
            return answer
        before, rhs_now = made[2:4]
        diag_now = diag_next
        if level < steps - 1:
            diag_next, off_now = made[4:6]
        if level == 1:
            labels = made[-1]
        arrived = exchange(made[1].reshape(owners, chunk, width))
        arrived = arrived.reshape(owners * CAP, rows, width)


def solution(mesh):
    spread = P(None, AXES)
    return jax.shard_map(
        shards,
        mesh=mesh,
        in_specs=(P(None, AXES, None, None),) * 3 + (spread,) * 4,
        out_specs=P(None, AXES, None, None),
        check_vma=False,
    )
```

```python
import functools

import jax
import jax.numpy as jnp
from jax import lax
from jax.experimental import pallas as pl
from jax.experimental.pallas import tpu as pltpu
from jax.sharding import PartitionSpec as P

CAP = 2
AXES = ("gx", "gy", "gz")
VMEM = pl.BlockSpec(memory_space=pltpu.VMEM)
SMEM = pl.BlockSpec(memory_space=pltpu.SMEM)
HBM = pl.BlockSpec(memory_space=pltpu.HBM)
PARAMS = pltpu.CompilerParams(vmem_limit_bytes=16 * 1024 * 1024)
PIECES = 4


class Copies:
    def __init__(self, sems):
        self.sems, self.used = sems, 0

    def start(self, source, target):
        copy = pltpu.make_async_copy(source, target, self.sems.at[self.used])
        self.used += 1
        copy.start()
        return copy


def wait(*copies):
    for copy in copies:
        copy.wait()


def pieces(count):
    size = -(-count // (2 * PIECES)) * 2
    return [(at, min(size, count - at)) for at in range(0, count, size)]


def products(left, blocks, start, count):
    found = []
    rows, width = left(0).shape
    none = jnp.zeros((rows, width), jnp.float32)
    for at in range(0, count - 1, 2):
        upper = jnp.concatenate([left(at), none], axis=0).astype(jnp.bfloat16)
        lower = jnp.concatenate([none, left(at + 1)], axis=0).astype(jnp.bfloat16)
        pair = blocks[start + at : start + at + 2].reshape(2 * width, width)
        both = jnp.dot(jnp.concatenate([upper, lower], axis=1), pair, preferred_element_type=jnp.float32)
        found += [both[:rows], both[rows:]]
    if count % 2:
        one = left(count - 1).astype(jnp.bfloat16)
        found.append(jnp.dot(one, blocks[start + count - 1], preferred_element_type=jnp.float32))
    return found


def solve(live_count, work_of, diag, solved):
    for slot, out in enumerate(products(work_of, diag, 0, solved.shape[0])):
        solved[slot] = jnp.where(slot < live_count, out, jnp.zeros_like(out))


def first_kernel(owners, *refs):
    live, source, target, block, rhs, diag, off = refs[:7]
    outgoing, solved, live_now, source_now, place = refs[7:12]
    target_now, owner_rows, block_rows, taken, rhs_now, diag_now, off_now, sems = refs[12:]
    copies = Copies(sems)
    tables = [
        copies.start(target, target_now),
        copies.start(target, owner_rows),
        copies.start(block, block_rows),
        copies.start(source, source_now),
        copies.start(live, live_now),
    ]
    load_rhs = copies.start(rhs.at[0], rhs_now)
    load_diag = copies.start(diag.at[0], diag_now)
    steps, records = owner_rows.shape
    slots, rows, width = solved.shape
    chunk = CAP * rows + 1
    out = outgoing.reshape(owners * chunk, width)
    parts = pieces(records)
    load_off = [copies.start(off.at[0, pl.ds(at, size)], off_now.at[pl.ds(at, size)]) for at, size in parts]
    wait(*tables)

    for level in range(steps):
        for owner in range(owners):
            taken[level, owner] = 0
    for record in range(records):
        for level in range(steps):
            owner = target_now[level, record]
            count = taken[level, owner]
            taken[level, owner] = count + 1
            if level == 0:
                place[level, record] = owner * chunk + count * rows
            else:
                place[level, record] = owner * CAP + count

    blocks = (steps + 1) * slots
    base = 1 << blocks.bit_length()
    none = jnp.float32(records * base)
    ids = lax.broadcasted_iota(jnp.int32, (owners, records), 0)
    order = lax.broadcasted_iota(jnp.int32, (owners, records), 1) * base
    lane = lax.broadcasted_iota(jnp.int32, (owners, width), 1)
    labels = jnp.zeros((owners, width), jnp.float32)
    for level in range(steps):
        hit = owner_rows[level : level + 1, :] == ids
        coded = (order + block_rows[level : level + 1, :]).astype(jnp.float32)
        low = jnp.min(jnp.where(hit, coded, none), axis=1, keepdims=True)
        high = jnp.max(jnp.where(hit, coded, jnp.float32(-1)), axis=1, keepdims=True)
        for at, value in enumerate((low, high)):
            label = (value.astype(jnp.int32) & (base - 1)).astype(jnp.float32)
            label = jnp.where(low < none, label, jnp.float32(blocks))
            labels = jnp.where(lane == level * CAP + at, label, labels)
    for owner in range(owners):
        out[owner * chunk + CAP * rows : (owner + 1) * chunk, :] = labels[owner : owner + 1, :]

    wait(load_rhs, load_diag)
    solve(live_now[0], lambda slot: rhs_now[slot], diag_now, solved)
    for (at, size), copy in zip(parts, load_off):
        copy.wait()
        values = products(lambda i: solved[source_now[0, at + i]], off_now, at, size)
        for record, value in enumerate(values, at):
            out[pl.ds(place[0, record], rows), :] = value


def work_of_level(level, levels, owners, at, copies):
    solved, labels, live = at["solved"], at["labels"], at["live"]
    slots, rows, width = solved.shape
    last = level == levels - 1
    left = levels - level
    chunk = CAP * rows
    totals = at["even"], at["odd"]
    if level == 1:
        gathered, turned = at["gathered"], at["turned"]
        flat = at["arrived"].reshape(owners * (chunk + 1), width)
        for owner in range(owners):
            row = owner * (chunk + 1) + chunk
            gathered[owner : owner + 1, :] = flat[row : row + 1, :]
        turned[...] = gathered[...].T[: turned.shape[0], :].astype(jnp.int32)
        copy = copies.start(turned, labels)
        totals[0][...] = jnp.zeros_like(totals[0])
        totals[1][...] = jnp.zeros_like(totals[1])
        copy.wait()
    else:
        totals[0][0 : left * slots] = at["before"][...]
        totals[1][...] = jnp.zeros_like(totals[1])
    for owner in range(owners):
        for which, total in enumerate(totals):
            label = labels[(level - 1) * CAP + which, owner] - level * slots
            if level == 1:
                start = owner * (chunk + 1) + which * rows
                value = flat[start : start + rows, :]
            else:
                value = at["arrived"][owner * CAP + which]
            total[label] += value
    rhs = at["rhs"].at[level]
    solve(live[level], lambda slot: rhs[slot] - (totals[0][slot] + totals[1][slot]), at["diag"].at[level], solved)
    if last:
        wait(copies.start(solved, at["answer"].at[level]))
    else:
        off = at["off"].at[level]
        values = products(lambda i: solved[at["source"][level, i]], off, 0, off.shape[0])
        for record, value in enumerate(values):
            at["outgoing"][at["place"][level, record]] = value
        at["after"][...] = totals[0][slots : left * slots] + totals[1][slots : left * slots]


def later_kernel(level, levels, owners, names, *refs):
    at = dict(zip(names, refs))
    last = level == levels - 1
    copies = Copies(at["sems"])
    live = at["live"]
    ahead = [copies.start(at["solved_before"], at["answer"].at[level - 1])]

    @pl.when(live[level] >= 0)
    def _():
        work_of_level(level, levels, owners, at, copies)

    wait(*ahead)


def shards(right_side, diag_inverse, off_blocks, live_counts, source_slot, target_owner, target_block):
    levels, slots, rows, width = right_side.shape
    records = off_blocks.shape[1]
    owners = lax.axis_size(AXES)
    steps = levels - 1
    chunk = CAP * rows
    f32, bf16, i32 = jnp.float32, jnp.bfloat16, jnp.int32
    near, table, semaphores = pltpu.VMEM, pltpu.SMEM, pltpu.SemaphoreType.DMA
    rows_shape = (slots, rows, width)
    diag_shape, off_shape = (slots, width, width), (records, width, width)
    arguments = (live_counts.reshape(levels), source_slot, target_owner, target_block)
    arguments += (right_side, diag_inverse, off_blocks)
    arguments = [pltpu.with_memory_space_constraint(x, pltpu.HBM) for x in arguments]
    rhs, diag, off = (
        pltpu.with_memory_space_constraint(x, pltpu.VMEM) for x in (right_side, diag_inverse, off_blocks)
    )

    def exchange(parts):
        return lax.all_to_all(parts, AXES, split_axis=0, concat_axis=0, tiled=True)

    outgoing, solved, live, source, place = pl.pallas_call(
        functools.partial(first_kernel, owners),
        out_shape=[
            near((owners * (chunk + 1), 1, width), f32),
            near(rows_shape, f32),
            table((levels,), i32),
            table((steps, records), i32),
            table((steps, records), i32),
        ],
        in_specs=[HBM] * 7,
        out_specs=[VMEM, VMEM, SMEM, SMEM, SMEM],
        scratch_shapes=[
            table((steps, records), i32),
            near((steps, records), i32),
            near((steps, records), i32),
            table((steps, owners), i32),
            near(rows_shape, f32),
            near(diag_shape, bf16),
            near(off_shape, bf16),
            semaphores((11 + PIECES,)),
        ],
        name="level_0",
        compiler_params=PARAMS,
    )(*arguments)
    arrived = exchange(outgoing.reshape(owners, chunk + 1, 1, width)).reshape(owners * (chunk + 1), 1, width)

    answer = labels = before = None
    for level in range(1, levels):
        last = level == levels - 1
        left = levels - level
        ins = [("live", live, SMEM), ("rhs", rhs, VMEM), ("diag", diag, VMEM), ("arrived", arrived, VMEM)]
        ins.append(("solved_before", solved, VMEM))
        outs = [("answer", pltpu.HBM((levels, *rows_shape), f32), HBM)]
        scratch = [("even", near((left * slots + 1, rows, width), f32)), ("odd", near((left * slots + 1, rows, width), f32))]
        scratch.append(("sems", semaphores((6,))))
        if level == 1:
            outs.append(("labels", table((steps * CAP, owners), i32), SMEM))
            scratch += [("gathered", near((owners, width), f32)), ("turned", near((steps * CAP, owners), i32))]
        else:
            ins += [("labels", labels, SMEM), ("before", before, VMEM)]
        if last:
            scratch.append(("solved", near(rows_shape, f32)))
        else:
            ins += [("source", source, SMEM), ("place", place, SMEM), ("off", off, VMEM)]
            outs.append(("solved", near(rows_shape, f32), VMEM))
            outs.append(("outgoing", near((owners * CAP, rows, width), f32), VMEM))
            outs.append(("after", near(((left - 1) * slots, rows, width), f32), VMEM))
        if level > 1:
            ins.append(("answer_before", pltpu.with_memory_space_constraint(answer, pltpu.HBM), HBM))
        names = [name for name, *_ in ins + outs + scratch]
        made = pl.pallas_call(
            functools.partial(later_kernel, level, levels, owners, names),
            out_shape=[shape for _, shape, _ in outs],
            in_specs=[spec for *_, spec in ins],
            out_specs=[spec for *_, spec in outs],
            input_output_aliases={len(ins) - 1: 0} if level > 1 else {},
            scratch_shapes=[shape for _, shape in scratch],
            name=f"level_{level}",
            compiler_params=PARAMS,
        )(*[value for _, value, _ in ins])
        made = dict(zip([name for name, *_ in outs], made))
        answer = made["answer"]
        if last:
            return answer
        solved, before = made["solved"], made["after"]
        labels = made.get("labels", labels)
        arrived = exchange(made["outgoing"].reshape(owners, chunk, width)).reshape(owners * CAP, rows, width)


def solution(mesh):
    spread = P(None, AXES)
    return jax.shard_map(
        shards,
        mesh=mesh,
        in_specs=(P(None, AXES, None, None),) * 3 + (spread,) * 4,
        out_specs=P(None, AXES, None, None),
        check_vma=False,
    )
```

```python
import functools

import jax
import jax.numpy as jnp
from jax import lax
from jax.experimental import pallas as pl
from jax.experimental.pallas import tpu as pltpu
from jax.sharding import PartitionSpec as P

CAP = 2
AXES = ("gx", "gy", "gz")
VMEM = pl.BlockSpec(memory_space=pltpu.VMEM)
SMEM = pl.BlockSpec(memory_space=pltpu.SMEM)
HBM = pl.BlockSpec(memory_space=pltpu.HBM)
PARAMS = pltpu.CompilerParams(vmem_limit_bytes=16 * 1024 * 1024)
PIECES = 4


class Copies:
    def __init__(self, sems):
        self.sems, self.used = sems, 0

    def make(self, source, target):
        self.used += 1
        return pltpu.make_async_copy(source, target, self.sems.at[self.used - 1])

    def start(self, source, target):
        copy = self.make(source, target)
        copy.start()
        return copy


def wait(*copies):
    for copy in copies:
        copy.wait()


def pieces(count):
    size = -(-count // (2 * PIECES)) * 2
    return [(at, min(size, count - at)) for at in range(0, count, size)]


def products(left, blocks, start, count):
    found = []
    rows, width = left(0).shape
    none = jnp.zeros((rows, width), jnp.float32)
    for at in range(0, count - 1, 2):
        upper = jnp.concatenate([left(at), none], axis=0).astype(jnp.bfloat16)
        lower = jnp.concatenate([none, left(at + 1)], axis=0).astype(jnp.bfloat16)
        pair = blocks[start + at : start + at + 2].reshape(2 * width, width)
        both = jnp.dot(jnp.concatenate([upper, lower], axis=1), pair, preferred_element_type=jnp.float32)
        found += [both[:rows], both[rows:]]
    if count % 2:
        one = left(count - 1).astype(jnp.bfloat16)
        found.append(jnp.dot(one, blocks[start + count - 1], preferred_element_type=jnp.float32))
    return found


def solve(live_count, work_of, diag, solved):
    for slot, out in enumerate(products(work_of, diag, 0, solved.shape[0])):
        solved[slot] = jnp.where(slot < live_count, out, jnp.zeros_like(out))


def first_kernel(owners, *refs):
    live, source, target, block, rhs, diag, off = refs[:7]
    outgoing, solved, live_now, source_now, place = refs[7:12]
    owner_rows, block_rows, place_rows, rhs_now, diag_now, off_now, sems = refs[12:]
    copies = Copies(sems)
    tables = [copies.start(target, owner_rows), copies.start(block, block_rows)]
    scalars = [copies.start(source, source_now), copies.start(live, live_now)]
    load_rhs = copies.start(rhs.at[0], rhs_now)
    load_diag = copies.start(diag.at[0], diag_now)
    steps, records = owner_rows.shape
    slots, rows, width = solved.shape
    chunk = CAP * rows + 1
    out = outgoing.reshape(owners * chunk, width)
    parts = pieces(records)
    load_off = [copies.start(off.at[0, pl.ds(at, size)], off_now.at[pl.ds(at, size)]) for at, size in parts]
    wait(*tables)

    blocks = (steps + 1) * slots
    base = 1 << blocks.bit_length()
    none = jnp.float32(records * base)
    ids = lax.broadcasted_iota(jnp.int32, (owners, records), 0)
    order = lax.broadcasted_iota(jnp.int32, (owners, records), 1) * base
    lane = lax.broadcasted_iota(jnp.int32, (owners, width), 1)
    labels = jnp.zeros((owners, width), jnp.float32)
    for level in range(steps):
        hit = owner_rows[level : level + 1, :] == ids
        coded = (order + block_rows[level : level + 1, :]).astype(jnp.float32)
        low = jnp.min(jnp.where(hit, coded, none), axis=1, keepdims=True)
        high = jnp.max(jnp.where(hit, coded, jnp.float32(-1)), axis=1, keepdims=True)
        is_first = jnp.where(hit & (coded == low), jnp.float32(1), jnp.float32(0))
        second = 1 - jnp.sum(is_first, axis=0, keepdims=True).astype(jnp.int32)
        owner_row = owner_rows[level : level + 1, :]
        place_rows[level : level + 1, :] = owner_row * (CAP if level else chunk) + second * (1 if level else rows)
        for at, value in enumerate((low, high)):
            label = (value.astype(jnp.int32) & (base - 1)).astype(jnp.float32)
            label = jnp.where(low < none, label, jnp.float32(blocks))
            labels = jnp.where(lane == level * CAP + at, label, labels)
    keep_place = copies.start(place_rows, place)
    for owner in range(owners):
        out[owner * chunk + CAP * rows : (owner + 1) * chunk, :] = labels[owner : owner + 1, :]

    wait(load_rhs, load_diag, *scalars)
    solve(live_now[0], lambda slot: rhs_now[slot], diag_now, solved)
    keep_place.wait()
    for (at, size), copy in zip(parts, load_off):
        copy.wait()
        values = products(lambda i: solved[source_now[0, at + i]], off_now, at, size)
        for record, value in enumerate(values, at):
            out[pl.ds(place[0, record], rows), :] = value


def add_arrived(level, levels, owners, at, keep_labels):
    labels = at["labels"]
    slots, rows, width = at["solved"].shape
    left = levels - level
    chunk = CAP * rows
    totals = at["even"], at["odd"]
    if level == 1:
        flat = at["arrived"].reshape(owners * (chunk + 1), width)
        totals[0][...] = jnp.zeros_like(totals[0])
        totals[1][...] = jnp.zeros_like(totals[1])
    else:
        totals[0][0 : left * slots] = at["before"][...]
        totals[1][...] = jnp.zeros_like(totals[1])
    for owner in range(owners):
        if level == 1:
            row = owner * (chunk + 1) + chunk
            sent = flat[row : row + 1, :].astype(jnp.int32) - level * slots
        for which, total in enumerate(totals):
            if level == 1:
                label = sent[0, which]
            else:
                label = labels[(level - 1) * CAP + which, owner] - level * slots
            if level == 1:
                start = owner * (chunk + 1) + which * rows
                value = flat[start : start + rows, :]
            else:
                value = at["arrived"][owner * CAP + which]
            total[label] += value
    if level == 1:
        gathered, turned = at["gathered"], at["turned"]
        for owner in range(owners):
            row = owner * (chunk + 1) + chunk
            gathered[owner : owner + 1, :] = flat[row : row + 1, :]
        turned[...] = gathered[...].T[: turned.shape[0], :].astype(jnp.int32)
        keep_labels.start()


def solve_and_pack(level, levels, at, copies):
    solved, live, totals = at["solved"], at["live"], (at["even"], at["odd"])
    slots = solved.shape[0]
    last = level == levels - 1
    left = levels - level
    rhs = at["rhs"].at[level]
    solve(live[level], lambda slot: rhs[slot] - (totals[0][slot] + totals[1][slot]), at["diag"].at[level], solved)
    if last:
        wait(copies.start(solved, at["answer"].at[level]))
    else:
        off = at["off"].at[level]
        values = products(lambda i: solved[at["source"][level, i]], off, 0, off.shape[0])
        for record, value in enumerate(values):
            at["outgoing"][at["place"][level, record]] = value
        at["after"][...] = totals[0][slots : left * slots] + totals[1][slots : left * slots]


def later_kernel(level, levels, owners, names, *refs):
    at = dict(zip(names, refs))
    copies = Copies(at["sems"])
    live = at["live"]
    ahead = [copies.start(at["solved_before"], at["answer"].at[level - 1])]

    keep_labels = copies.make(at["turned"], at["labels"]) if level == 1 else None

    @pl.when(live[level] >= 0)
    def _():
        add_arrived(level, levels, owners, at, keep_labels)

    @pl.when(live[level] >= 0)
    def _():
        solve_and_pack(level, levels, at, copies)

    wait(*ahead, *([keep_labels] if level == 1 else []))


def shards(right_side, diag_inverse, off_blocks, live_counts, source_slot, target_owner, target_block):
    levels, slots, rows, width = right_side.shape
    records = off_blocks.shape[1]
    owners = lax.axis_size(AXES)
    steps = levels - 1
    chunk = CAP * rows
    f32, bf16, i32 = jnp.float32, jnp.bfloat16, jnp.int32
    near, table, semaphores = pltpu.VMEM, pltpu.SMEM, pltpu.SemaphoreType.DMA
    rows_shape = (slots, rows, width)
    diag_shape, off_shape = (slots, width, width), (records, width, width)
    arguments = (live_counts.reshape(levels), source_slot, target_owner, target_block)
    arguments += (right_side, diag_inverse, off_blocks)
    arguments = [pltpu.with_memory_space_constraint(x, pltpu.HBM) for x in arguments]
    rhs, diag, off = (
        pltpu.with_memory_space_constraint(x, pltpu.VMEM) for x in (right_side, diag_inverse, off_blocks)
    )

    def exchange(parts):
        return lax.all_to_all(parts, AXES, split_axis=0, concat_axis=0, tiled=True)

    outgoing, solved, live, source, place = pl.pallas_call(
        functools.partial(first_kernel, owners),
        out_shape=[
            near((owners * (chunk + 1), 1, width), f32),
            near(rows_shape, f32),
            table((levels,), i32),
            table((steps, records), i32),
            table((steps, records), i32),
        ],
        in_specs=[HBM] * 7,
        out_specs=[VMEM, VMEM, SMEM, SMEM, SMEM],
        scratch_shapes=[
            near((steps, records), i32),
            near((steps, records), i32),
            near((steps, records), i32),
            near(rows_shape, f32),
            near(diag_shape, bf16),
            near(off_shape, bf16),
            semaphores((11 + PIECES,)),
        ],
        name="level_0",
        compiler_params=PARAMS,
    )(*arguments)
    arrived = exchange(outgoing.reshape(owners, chunk + 1, 1, width)).reshape(owners * (chunk + 1), 1, width)

    answer = labels = before = None
    for level in range(1, levels):
        last = level == levels - 1
        left = levels - level
        ins = [("live", live, SMEM), ("rhs", rhs, VMEM), ("diag", diag, VMEM), ("arrived", arrived, VMEM)]
        ins.append(("solved_before", solved, VMEM))
        outs = [("answer", pltpu.HBM((levels, *rows_shape), f32), HBM)]
        scratch = [("even", near((left * slots + 1, rows, width), f32)), ("odd", near((left * slots + 1, rows, width), f32))]
        scratch.append(("sems", semaphores((6,))))
        if level == 1:
            outs.append(("labels", table((steps * CAP, owners), i32), SMEM))
            scratch += [("gathered", near((owners, width), f32)), ("turned", near((steps * CAP, owners), i32))]
        else:
            ins += [("labels", labels, SMEM), ("before", before, VMEM)]
        if last:
            scratch.append(("solved", near(rows_shape, f32)))
        else:
            ins += [("source", source, SMEM), ("place", place, SMEM), ("off", off, VMEM)]
            outs.append(("solved", near(rows_shape, f32), VMEM))
            outs.append(("outgoing", near((owners * CAP, rows, width), f32), VMEM))
            outs.append(("after", near(((left - 1) * slots, rows, width), f32), VMEM))
        if level > 1:
            ins.append(("answer_before", pltpu.with_memory_space_constraint(answer, pltpu.HBM), HBM))
        names = [name for name, *_ in ins + outs + scratch]
        made = pl.pallas_call(
            functools.partial(later_kernel, level, levels, owners, names),
            out_shape=[shape for _, shape, _ in outs],
            in_specs=[spec for *_, spec in ins],
            out_specs=[spec for *_, spec in outs],
            input_output_aliases={len(ins) - 1: 0} if level > 1 else {},
            scratch_shapes=[shape for _, shape in scratch],
            name=f"level_{level}",
            compiler_params=PARAMS,
        )(*[value for _, value, _ in ins])
        made = dict(zip([name for name, *_ in outs], made))
        answer = made["answer"]
        if last:
            return answer
        solved, before = made["solved"], made["after"]
        labels = made.get("labels", labels)
        arrived = exchange(made["outgoing"].reshape(owners, chunk, width)).reshape(owners * CAP, rows, width)


def solution(mesh):
    spread = P(None, AXES)
    return jax.shard_map(
        shards,
        mesh=mesh,
        in_specs=(P(None, AXES, None, None),) * 3 + (spread,) * 4,
        out_specs=P(None, AXES, None, None),
        check_vma=False,
    )
```

```python
import functools

import jax
import jax.numpy as jnp
from jax import lax
from jax.experimental import pallas as pl
from jax.experimental.pallas import tpu as pltpu
from jax.sharding import PartitionSpec as P

CAP = 2
AXES = ("gx", "gy", "gz")
VMEM = pl.BlockSpec(memory_space=pltpu.VMEM)
SMEM = pl.BlockSpec(memory_space=pltpu.SMEM)
HBM = pl.BlockSpec(memory_space=pltpu.HBM)
PARAMS = pltpu.CompilerParams(vmem_limit_bytes=16 * 1024 * 1024)


class Copies:
    def __init__(self, sems):
        self.sems, self.used = sems, 0

    def make(self, source, target):
        self.used += 1
        return pltpu.make_async_copy(source, target, self.sems.at[self.used - 1])

    def start(self, source, target):
        copy = self.make(source, target)
        copy.start()
        return copy


def wait(*copies):
    for copy in copies:
        copy.wait()


def products(left, blocks, start, count):
    found = []
    rows, width = left(0).shape
    none = jnp.zeros((rows, width), jnp.float32)
    for at in range(0, count - 1, 2):
        upper = jnp.concatenate([left(at), none], axis=0).astype(jnp.bfloat16)
        lower = jnp.concatenate([none, left(at + 1)], axis=0).astype(jnp.bfloat16)
        pair = blocks[start + at : start + at + 2].reshape(2 * width, width)
        both = jnp.dot(jnp.concatenate([upper, lower], axis=1), pair, preferred_element_type=jnp.float32)
        found += [both[:rows], both[rows:]]
    if count % 2:
        one = left(count - 1).astype(jnp.bfloat16)
        found.append(jnp.dot(one, blocks[start + count - 1], preferred_element_type=jnp.float32))
    return found


def solve(live_count, work_of, diag, solved):
    for slot, out in enumerate(products(work_of, diag, 0, solved.shape[0])):
        solved[slot] = jnp.where(slot < live_count, out, jnp.zeros_like(out))


def first_kernel(owners, *refs):
    live, source, target, block, rhs, diag, off = refs[:7]
    outgoing, solved, live_now, source_now, place = refs[7:12]
    owner_rows, block_rows, place_rows, rhs_now, diag_now, off_now, sems = refs[12:]
    copies = Copies(sems)
    tables = [copies.start(target, owner_rows), copies.start(block, block_rows)]
    load_diag = copies.start(diag.at[0], diag_now)
    load_rhs = copies.start(rhs.at[0], rhs_now)
    scalars = [copies.start(live, live_now), copies.start(source, source_now)]
    steps, records = owner_rows.shape
    slots, rows, width = solved.shape
    chunk = CAP * rows + 1
    out = outgoing.reshape(owners * chunk, width)
    load_off = copies.start(off.at[0], off_now)
    wait(*tables)

    blocks = (steps + 1) * slots
    base = 1 << blocks.bit_length()
    none = jnp.float32(records * base)
    ids = lax.broadcasted_iota(jnp.int32, (owners, records), 0)
    order = lax.broadcasted_iota(jnp.int32, (owners, records), 1) * base
    lane = lax.broadcasted_iota(jnp.int32, (owners, width), 1)
    labels = jnp.zeros((owners, width), jnp.float32)
    for level in range(steps):
        hit = owner_rows[level : level + 1, :] == ids
        coded = (order + block_rows[level : level + 1, :]).astype(jnp.float32)
        low = jnp.min(jnp.where(hit, coded, none), axis=1, keepdims=True)
        high = jnp.max(jnp.where(hit, coded, jnp.float32(-1)), axis=1, keepdims=True)
        is_first = jnp.where(hit & (coded == low), jnp.float32(1), jnp.float32(0))
        second = 1 - jnp.sum(is_first, axis=0, keepdims=True).astype(jnp.int32)
        owner_row = owner_rows[level : level + 1, :]
        place_rows[level : level + 1, :] = owner_row * (CAP if level else chunk) + second * (1 if level else rows)
        for at, value in enumerate((low, high)):
            label = (value.astype(jnp.int32) & (base - 1)).astype(jnp.float32)
            label = jnp.where(low < none, label, jnp.float32(blocks))
            labels = jnp.where(lane == level * CAP + at, label, labels)
    keep_place = copies.start(place_rows, place)
    for owner in range(owners):
        out[owner * chunk + CAP * rows : (owner + 1) * chunk, :] = labels[owner : owner + 1, :]

    wait(load_rhs, load_diag, *scalars)
    solve(live_now[0], lambda slot: rhs_now[slot], diag_now, solved)
    wait(keep_place, load_off)
    values = products(lambda i: solved[source_now[0, i]], off_now, 0, records)
    for record, value in enumerate(values):
        out[pl.ds(place[0, record], rows), :] = value


def chains(level):
    return [f"total_{at}" for at in range(2 if level == 1 else 4)]


def add_arrived(level, levels, owners, at, keep_labels):
    labels = at["labels"]
    slots, rows, width = at["solved"].shape
    left = levels - level
    chunk = CAP * rows
    totals = [at[name] for name in chains(level)]
    for total in totals:
        total[...] = jnp.zeros_like(total)
    if level == 1:
        flat = at["arrived"].reshape(owners * (chunk + 1), width)
    else:
        totals[0][0 : left * slots] = at["before"][...]
    for owner in range(owners):
        if level == 1:
            row = owner * (chunk + 1) + chunk
            sent = flat[row : row + 1, :].astype(jnp.int32) - level * slots
        for which in range(CAP):
            total = totals[(owner * CAP + which) % len(totals)]
            if level == 1:
                label = sent[0, which]
            else:
                label = labels[(level - 1) * CAP + which, owner] - level * slots
            if level == 1:
                start = owner * (chunk + 1) + which * rows
                value = flat[start : start + rows, :]
            else:
                value = at["arrived"][owner * CAP + which]
            total[label] += value
    if level == 1:
        gathered, turned = at["gathered"], at["turned"]
        for owner in range(owners):
            row = owner * (chunk + 1) + chunk
            gathered[owner : owner + 1, :] = flat[row : row + 1, :]
        turned[...] = gathered[...].T[: turned.shape[0], :].astype(jnp.int32)
        keep_labels.start()


def solve_and_pack(level, levels, at, copies):
    solved, live = at["solved"], at["live"]
    slots = solved.shape[0]
    last = level == levels - 1
    left = levels - level
    rhs = at["rhs"].at[level]
    totals = [at[name] for name in chains(level)]

    def total_of(part):
        return sum((total[part] for total in totals[1:]), totals[0][part])

    solve(live[level], lambda slot: rhs[slot] - total_of(slot), at["diag"].at[level], solved)
    if last:
        wait(copies.start(solved, at["answer"].at[level]))
    else:
        off = at["off"].at[level]
        values = products(lambda i: solved[at["source"][level, i]], off, 0, off.shape[0])
        for record, value in enumerate(values):
            at["outgoing"][at["place"][level, record]] = value
        at["after"][...] = total_of(slice(slots, left * slots))


def later_kernel(level, levels, owners, names, *refs):
    at = dict(zip(names, refs))
    copies = Copies(at["sems"])
    live = at["live"]
    ahead = []
    if level == levels - 1:
        ahead = [copies.start(at[f"solved_{before}"], at["answer"].at[before]) for before in range(level)]

    keep_labels = copies.make(at["turned"], at["labels"]) if level == 1 else None

    @pl.when(live[level] >= 0)
    def _():
        add_arrived(level, levels, owners, at, keep_labels)

    @pl.when(live[level] >= 0)
    def _():
        solve_and_pack(level, levels, at, copies)

    wait(*ahead, *([keep_labels] if level == 1 else []))


def shards(right_side, diag_inverse, off_blocks, live_counts, source_slot, target_owner, target_block):
    levels, slots, rows, width = right_side.shape
    records = off_blocks.shape[1]
    owners = lax.axis_size(AXES)
    steps = levels - 1
    chunk = CAP * rows
    f32, bf16, i32 = jnp.float32, jnp.bfloat16, jnp.int32
    near, table, semaphores = pltpu.VMEM, pltpu.SMEM, pltpu.SemaphoreType.DMA
    rows_shape = (slots, rows, width)
    diag_shape, off_shape = (slots, width, width), (records, width, width)
    arguments = (live_counts.reshape(levels), source_slot, target_owner, target_block)
    arguments += (right_side, diag_inverse, off_blocks)
    arguments = [pltpu.with_memory_space_constraint(x, pltpu.HBM) for x in arguments]
    rhs, diag, off = (
        pltpu.with_memory_space_constraint(x, pltpu.VMEM) for x in (right_side, diag_inverse, off_blocks)
    )

    def exchange(parts):
        return lax.all_to_all(parts, AXES, split_axis=0, concat_axis=0, tiled=True)

    outgoing, solved, live, source, place = pl.pallas_call(
        functools.partial(first_kernel, owners),
        out_shape=[
            near((owners * (chunk + 1), 1, width), f32),
            near(rows_shape, f32),
            table((levels,), i32),
            table((steps, records), i32),
            table((steps, records), i32),
        ],
        in_specs=[HBM] * 7,
        out_specs=[VMEM, VMEM, SMEM, SMEM, SMEM],
        scratch_shapes=[
            near((steps, records), i32),
            near((steps, records), i32),
            near((steps, records), i32),
            near(rows_shape, f32),
            near(diag_shape, bf16),
            near(off_shape, bf16),
            semaphores((8,)),
        ],
        name="level_0",
        compiler_params=PARAMS,
    )(*arguments)
    arrived = exchange(outgoing.reshape(owners, chunk + 1, 1, width)).reshape(owners * (chunk + 1), 1, width)

    solved = [solved]
    labels = before = None
    for level in range(1, levels):
        last = level == levels - 1
        left = levels - level
        ins = [("live", live, SMEM), ("rhs", rhs, VMEM), ("diag", diag, VMEM), ("arrived", arrived, VMEM)]
        outs = []
        scratch = [(name, near((left * slots + 1, rows, width), f32)) for name in chains(level)]
        scratch.append(("sems", semaphores((levels + 1,))))
        if level == 1:
            outs.append(("labels", table((steps * CAP, owners), i32), SMEM))
            scratch += [("gathered", near((owners, width), f32)), ("turned", near((steps * CAP, owners), i32))]
        else:
            ins += [("labels", labels, SMEM), ("before", before, VMEM)]
        if last:
            ins += [(f"solved_{before}", value, VMEM) for before, value in enumerate(solved)]
            outs.append(("answer", pltpu.HBM((levels, *rows_shape), f32), HBM))
            scratch.append(("solved", near(rows_shape, f32)))
        else:
            ins += [("source", source, SMEM), ("place", place, SMEM), ("off", off, VMEM)]
            outs.append(("solved", near(rows_shape, f32), VMEM))
            outs.append(("outgoing", near((owners * CAP, rows, width), f32), VMEM))
            outs.append(("after", near(((left - 1) * slots, rows, width), f32), VMEM))
        names = [name for name, *_ in ins + outs + scratch]
        made = pl.pallas_call(
            functools.partial(later_kernel, level, levels, owners, names),
            out_shape=[shape for _, shape, _ in outs],
            in_specs=[spec for *_, spec in ins],
            out_specs=[spec for *_, spec in outs],
            scratch_shapes=[shape for _, shape in scratch],
            name=f"level_{level}",
            compiler_params=PARAMS,
        )(*[value for _, value, _ in ins])
        made = dict(zip([name for name, *_ in outs], made))
        if last:
            return made["answer"]
        solved.append(made["solved"])
        before = made["after"]
        labels = made.get("labels", labels)
        arrived = exchange(made["outgoing"].reshape(owners, chunk, width)).reshape(owners * CAP, rows, width)


def solution(mesh):
    spread = P(None, AXES)
    return jax.shard_map(
        shards,
        mesh=mesh,
        in_specs=(P(None, AXES, None, None),) * 3 + (spread,) * 4,
        out_specs=P(None, AXES, None, None),
        check_vma=False,
    )
```

```python
import functools

import jax
import jax.numpy as jnp
from jax import lax
from jax.experimental import pallas as pl
from jax.experimental.pallas import tpu as pltpu
from jax.sharding import PartitionSpec as P

CAP = 2
AXES = ("gx", "gy", "gz")
VMEM = pl.BlockSpec(memory_space=pltpu.VMEM)
SMEM = pl.BlockSpec(memory_space=pltpu.SMEM)
HBM = pl.BlockSpec(memory_space=pltpu.HBM)
PARAMS = pltpu.CompilerParams(vmem_limit_bytes=16 * 1024 * 1024)


class Copies:
    def __init__(self, sems):
        self.sems, self.used = sems, 0

    def make(self, source, target):
        self.used += 1
        return pltpu.make_async_copy(source, target, self.sems.at[self.used - 1])

    def start(self, source, target):
        copy = self.make(source, target)
        copy.start()
        return copy


def wait(*copies):
    for copy in copies:
        copy.wait()


def products(left, blocks, start, count):
    found = []
    rows, width = left(0).shape
    none = jnp.zeros((rows, width), jnp.float32)
    for at in range(0, count - 1, 2):
        upper = jnp.concatenate([left(at), none], axis=0).astype(jnp.bfloat16)
        lower = jnp.concatenate([none, left(at + 1)], axis=0).astype(jnp.bfloat16)
        pair = blocks[start + at : start + at + 2].reshape(2 * width, width)
        both = jnp.dot(jnp.concatenate([upper, lower], axis=1), pair, preferred_element_type=jnp.float32)
        found += [both[:rows], both[rows:]]
    if count % 2:
        one = left(count - 1).astype(jnp.bfloat16)
        found.append(jnp.dot(one, blocks[start + count - 1], preferred_element_type=jnp.float32))
    return found


def solve(live_count, work_of, diag, solved):
    for slot, out in enumerate(products(work_of, diag, 0, solved.shape[0])):
        solved[slot] = jnp.where(slot < live_count, out, jnp.zeros_like(out))


def first_kernel(owners, *refs):
    live, source, target, block, rhs, diag, off = refs[:7]
    outgoing, solved, live_now, source_now, place = refs[7:12]
    owner_rows, block_rows, place_rows, rhs_now, diag_now, off_now, sems = refs[12:]
    copies = Copies(sems)
    tables = [copies.start(target, owner_rows), copies.start(block, block_rows)]
    load_diag = copies.start(diag.at[0], diag_now)
    load_rhs = copies.start(rhs.at[0], rhs_now)
    scalars = [copies.start(live, live_now), copies.start(source, source_now)]
    steps, records = owner_rows.shape
    slots, rows, width = solved.shape
    chunk = CAP * rows + 1
    out = outgoing.reshape(owners * chunk, width)
    load_off = copies.start(off.at[0], off_now)
    wait(*tables)

    blocks = (steps + 1) * slots
    base = 1 << blocks.bit_length()
    none = jnp.float32(records * base)
    ids = lax.broadcasted_iota(jnp.int32, (owners, records), 0)
    order = lax.broadcasted_iota(jnp.int32, (owners, records), 1) * base
    lane = lax.broadcasted_iota(jnp.int32, (owners, width), 1)
    labels = jnp.zeros((owners, width), jnp.float32)
    for level in range(steps):
        hit = owner_rows[level : level + 1, :] == ids
        coded = (order + block_rows[level : level + 1, :]).astype(jnp.float32)
        low = jnp.min(jnp.where(hit, coded, none), axis=1, keepdims=True)
        high = jnp.max(jnp.where(hit, coded, jnp.float32(-1)), axis=1, keepdims=True)
        is_first = jnp.where(hit & (coded == low), jnp.float32(1), jnp.float32(0))
        second = 1 - jnp.sum(is_first, axis=0, keepdims=True).astype(jnp.int32)
        owner_row = owner_rows[level : level + 1, :]
        place_rows[level : level + 1, :] = owner_row * (CAP if level else chunk) + second * (1 if level else rows)
        for at, value in enumerate((low, high)):
            label = (value.astype(jnp.int32) & (base - 1)).astype(jnp.float32)
            label = jnp.where(low < none, label, jnp.float32(blocks))
            labels = jnp.where(lane == level * CAP + at, label, labels)
    keep_place = pltpu.make_async_copy(place_rows, place, sems.at[0])
    keep_place.start()
    for owner in range(owners):
        out[owner * chunk + CAP * rows : (owner + 1) * chunk, :] = labels[owner : owner + 1, :]

    wait(load_rhs, load_diag, *scalars)
    solve(live_now[0], lambda slot: rhs_now[slot], diag_now, solved)
    wait(keep_place, load_off)
    values = products(lambda i: solved[source_now[0, i]], off_now, 0, records)
    for record, value in enumerate(values):
        out[pl.ds(place[0, record], rows), :] = value


def chains(level):
    return [f"total_{at}" for at in range(2 if level == 1 else 4)]


def add_arrived(level, levels, owners, at, keep_labels):
    labels = at["labels"]
    slots, rows, width = at["solved"].shape
    left = levels - level
    chunk = CAP * rows
    totals = [at[name] for name in chains(level)]
    for total in totals:
        total[...] = jnp.zeros_like(total)
    if level == 1:
        flat = at["arrived"].reshape(owners * (chunk + 1), width)
    else:
        totals[0][0 : left * slots] = at["before"][...]
    for owner in range(owners):
        if level == 1:
            row = owner * (chunk + 1) + chunk
            sent = flat[row : row + 1, :].astype(jnp.int32) - level * slots
        for which in range(CAP):
            total = totals[(owner * CAP + which) % len(totals)]
            if level == 1:
                label = sent[0, which]
            else:
                label = labels[(level - 1) * CAP + which, owner] - level * slots
            if level == 1:
                start = owner * (chunk + 1) + which * rows
                value = flat[start : start + rows, :]
            else:
                value = at["arrived"][owner * CAP + which]
            total[label] += value
    if level == 1:
        gathered, turned = at["gathered"], at["turned"]
        for owner in range(owners):
            row = owner * (chunk + 1) + chunk
            gathered[owner : owner + 1, :] = flat[row : row + 1, :]
        turned[...] = gathered[...].T[: turned.shape[0], :].astype(jnp.int32)
        keep_labels.start()


def solve_and_pack(level, levels, at, copies):
    solved, live = at["solved"], at["live"]
    slots = solved.shape[0]
    last = level == levels - 1
    left = levels - level
    rhs = at["rhs"].at[level]
    totals = [at[name] for name in chains(level)]

    def total_of(part):
        return sum((total[part] for total in totals[1:]), totals[0][part])

    solve(live[level], lambda slot: rhs[slot] - total_of(slot), at["diag"].at[level], solved)
    if last:
        wait(copies.start(solved, at["answer"].at[level]))
    else:
        off = at["off"].at[level]
        values = products(lambda i: solved[at["source"][level, i]], off, 0, off.shape[0])
        for record, value in enumerate(values):
            at["outgoing"][at["place"][level, record]] = value
        at["after"][...] = total_of(slice(slots, left * slots))


def later_kernel(level, levels, owners, names, *refs):
    at = dict(zip(names, refs))
    copies = Copies(at.get("sems"))
    live = at["live"]
    ahead = []
    if level == levels - 1:
        ahead = [copies.start(at[f"solved_{before}"], at["answer"].at[before]) for before in range(level)]

    keep_labels = copies.make(at["turned"], at["labels"]) if level == 1 else None

    @pl.when(live[level] >= 0)
    def _():
        add_arrived(level, levels, owners, at, keep_labels)

    @pl.when(live[level] >= 0)
    def _():
        solve_and_pack(level, levels, at, copies)

    wait(*ahead, *([keep_labels] if level == 1 else []))


def shards(right_side, diag_inverse, off_blocks, live_counts, source_slot, target_owner, target_block):
    levels, slots, rows, width = right_side.shape
    records = off_blocks.shape[1]
    owners = lax.axis_size(AXES)
    steps = levels - 1
    chunk = CAP * rows
    f32, bf16, i32 = jnp.float32, jnp.bfloat16, jnp.int32
    near, table, semaphores = pltpu.VMEM, pltpu.SMEM, pltpu.SemaphoreType.DMA
    rows_shape = (slots, rows, width)
    diag_shape, off_shape = (slots, width, width), (records, width, width)
    arguments = (live_counts.reshape(levels), source_slot, target_owner, target_block)
    arguments += (right_side, diag_inverse, off_blocks)
    arguments = [pltpu.with_memory_space_constraint(x, pltpu.HBM) for x in arguments]
    rhs, diag, off = (
        pltpu.with_memory_space_constraint(x, pltpu.VMEM) for x in (right_side, diag_inverse, off_blocks)
    )

    def exchange(parts):
        return lax.all_to_all(parts, AXES, split_axis=0, concat_axis=0, tiled=True)

    outgoing, solved, live, source, place = pl.pallas_call(
        functools.partial(first_kernel, owners),
        out_shape=[
            near((owners * (chunk + 1), 1, width), f32),
            near(rows_shape, f32),
            table((levels,), i32),
            table((steps, records), i32),
            table((steps, records), i32),
        ],
        in_specs=[HBM] * 7,
        out_specs=[VMEM, VMEM, SMEM, SMEM, SMEM],
        scratch_shapes=[
            near((steps, records), i32),
            near((steps, records), i32),
            near((steps, records), i32),
            near(rows_shape, f32),
            near(diag_shape, bf16),
            near(off_shape, bf16),
            semaphores((7,)),
        ],
        name="level_0",
        compiler_params=PARAMS,
    )(*arguments)
    arrived = exchange(outgoing.reshape(owners, chunk + 1, 1, width)).reshape(owners * (chunk + 1), 1, width)

    solved = [solved]
    labels = before = None
    for level in range(1, levels):
        last = level == levels - 1
        left = levels - level
        ins = [("live", live, SMEM), ("rhs", rhs, VMEM), ("diag", diag, VMEM), ("arrived", arrived, VMEM)]
        outs = []
        scratch = [(name, near((left * slots + 1, rows, width), f32)) for name in chains(level)]
        if level == 1 or last:
            scratch.append(("sems", semaphores((levels if last else 1,))))
        if level == 1:
            outs.append(("labels", table((steps * CAP, owners), i32), SMEM))
            scratch += [("gathered", near((owners, width), f32)), ("turned", near((steps * CAP, owners), i32))]
        else:
            ins += [("labels", labels, SMEM), ("before", before, VMEM)]
        if last:
            ins += [(f"solved_{before}", value, VMEM) for before, value in enumerate(solved)]
            outs.append(("answer", pltpu.HBM((levels, *rows_shape), f32), HBM))
            scratch.append(("solved", near(rows_shape, f32)))
        else:
            ins += [("source", source, SMEM), ("place", place, SMEM), ("off", off, VMEM)]
            outs.append(("solved", near(rows_shape, f32), VMEM))
            outs.append(("outgoing", near((owners * CAP, rows, width), f32), VMEM))
            outs.append(("after", near(((left - 1) * slots, rows, width), f32), VMEM))
        names = [name for name, *_ in ins + outs + scratch]
        made = pl.pallas_call(
            functools.partial(later_kernel, level, levels, owners, names),
            out_shape=[shape for _, shape, _ in outs],
            in_specs=[spec for *_, spec in ins],
            out_specs=[spec for *_, spec in outs],
            scratch_shapes=[shape for _, shape in scratch],
            name=f"level_{level}",
            compiler_params=PARAMS,
        )(*[value for _, value, _ in ins])
        made = dict(zip([name for name, *_ in outs], made))
        if last:
            return made["answer"]
        solved.append(made["solved"])
        before = made["after"]
        labels = made.get("labels", labels)
        arrived = exchange(made["outgoing"].reshape(owners, chunk, width)).reshape(owners * CAP, rows, width)


def solution(mesh):
    spread = P(None, AXES)
    return jax.shard_map(
        shards,
        mesh=mesh,
        in_specs=(P(None, AXES, None, None),) * 3 + (spread,) * 4,
        out_specs=P(None, AXES, None, None),
        check_vma=False,
    )
```

```python
import functools

import jax
import jax.numpy as jnp
from jax import lax
from jax.experimental import pallas as pl
from jax.experimental.pallas import tpu as pltpu
from jax.sharding import PartitionSpec as P

CAP = 2
AXES = ("gx", "gy", "gz")
VMEM = pl.BlockSpec(memory_space=pltpu.VMEM)
SMEM = pl.BlockSpec(memory_space=pltpu.SMEM)
HBM = pl.BlockSpec(memory_space=pltpu.HBM)
PARAMS = pltpu.CompilerParams(vmem_limit_bytes=16 * 1024 * 1024)


class Copies:
    def __init__(self, sems):
        self.sems, self.used = sems, 0

    def make(self, source, target):
        self.used += 1
        return pltpu.make_async_copy(source, target, self.sems.at[self.used - 1])

    def start(self, source, target):
        copy = self.make(source, target)
        copy.start()
        return copy


def wait(*copies):
    for copy in copies:
        copy.wait()


def products(left, blocks, start, count):
    found = []
    rows, width = left(0).shape
    none = jnp.zeros((rows, width), jnp.float32)
    for at in range(0, count - 1, 2):
        upper = jnp.concatenate([left(at), none], axis=0).astype(jnp.bfloat16)
        lower = jnp.concatenate([none, left(at + 1)], axis=0).astype(jnp.bfloat16)
        pair = blocks[start + at : start + at + 2].reshape(2 * width, width)
        both = jnp.dot(jnp.concatenate([upper, lower], axis=1), pair, preferred_element_type=jnp.float32)
        found += [both[:rows], both[rows:]]
    if count % 2:
        one = left(count - 1).astype(jnp.bfloat16)
        found.append(jnp.dot(one, blocks[start + count - 1], preferred_element_type=jnp.float32))
    return found


def solve(live_count, work_of, diag, solved):
    for slot, out in enumerate(products(work_of, diag, 0, solved.shape[0])):
        solved[slot] = jnp.where(slot < live_count, out, jnp.zeros_like(out))


def first_kernel(owners, *refs):
    live, source, target, block, rhs, diag, off = refs[:7]
    outgoing, solved, live_now, source_now, place = refs[7:12]
    owner_rows, block_rows, place_rows, rhs_now, diag_now, off_now, sems = refs[12:]
    copies = Copies(sems)
    tables = [copies.start(target, owner_rows), copies.start(block, block_rows)]
    load_diag = copies.start(diag.at[0], diag_now)
    load_rhs = copies.start(rhs.at[0], rhs_now)
    scalars = [copies.start(live, live_now), copies.start(source, source_now)]
    steps, records = owner_rows.shape
    slots, rows, width = solved.shape
    chunk = CAP * rows + 1
    out = outgoing.reshape(owners * chunk, width)
    load_off = copies.start(off.at[0], off_now)
    wait(*tables)

    blocks = (steps + 1) * slots
    base = 1 << blocks.bit_length()
    none = jnp.float32(records * base)
    ids = lax.broadcasted_iota(jnp.int32, (owners, records), 0)
    order = lax.broadcasted_iota(jnp.int32, (owners, records), 1) * base
    lane = lax.broadcasted_iota(jnp.int32, (owners, width), 1)
    labels = jnp.zeros((owners, width), jnp.float32)
    for level in range(steps):
        hit = owner_rows[level : level + 1, :] == ids
        coded = (order + block_rows[level : level + 1, :]).astype(jnp.float32)
        low = jnp.min(jnp.where(hit, coded, none), axis=1, keepdims=True)
        high = jnp.max(jnp.where(hit, coded, jnp.float32(-1)), axis=1, keepdims=True)
        is_first = jnp.where(hit & (coded == low), jnp.float32(1), jnp.float32(0))
        second = 1 - jnp.sum(is_first, axis=0, keepdims=True).astype(jnp.int32)
        owner_row = owner_rows[level : level + 1, :]
        place_rows[level : level + 1, :] = owner_row * (CAP if level else chunk) + second * (1 if level else rows)
        for at, value in enumerate((low, high)):
            label = (value.astype(jnp.int32) & (base - 1)).astype(jnp.float32)
            label = jnp.where(low < none, label, jnp.float32(blocks))
            labels = jnp.where(lane == level * CAP + at, label, labels)
    keep_place = pltpu.make_async_copy(place_rows, place, sems.at[0])
    keep_place.start()
    for owner in range(owners):
        out[owner * chunk + CAP * rows : (owner + 1) * chunk, :] = labels[owner : owner + 1, :]

    wait(load_rhs, load_diag, *scalars)
    solve(live_now[0], lambda slot: rhs_now[slot], diag_now, solved)
    wait(keep_place, load_off)
    values = products(lambda i: solved[source_now[0, i]], off_now, 0, records)
    for record, value in enumerate(values):
        out[pl.ds(place[0, record], rows), :] = value


def chains(level):
    return [f"total_{at}" for at in range(2 if level == 1 else 4)]


def add_arrived(level, levels, owners, at, keep_labels):
    labels = at["labels"]
    slots, rows, width = at["solved"].shape
    left = levels - level
    chunk = CAP * rows
    totals = [at[name] for name in chains(level)]
    for total in totals:
        total[...] = jnp.zeros_like(total)
    if level == 1:
        flat = at["arrived"].reshape(owners * (chunk + 1), width)
    else:
        totals[0][0 : left * slots] = at["before"][...]
    for owner in range(owners):
        if level == 1:
            row = owner * (chunk + 1) + chunk
            sent = flat[row : row + 1, :].astype(jnp.int32) - level * slots
        for which in range(CAP):
            total = totals[(owner * CAP + which) % len(totals)]
            if level == 1:
                label = sent[0, which]
            else:
                label = labels[(level - 1) * CAP + which, owner] - level * slots
            if level == 1:
                start = owner * (chunk + 1) + which * rows
                value = flat[start : start + rows, :]
            else:
                value = at["arrived"][owner * CAP + which]
            total[label] += value
    if level == 1:
        gathered, turned = at["gathered"], at["turned"]
        for owner in range(owners):
            row = owner * (chunk + 1) + chunk
            gathered[owner : owner + 1, :] = flat[row : row + 1, :]
        turned[...] = gathered[...].T[: turned.shape[0], :].astype(jnp.int32)
        keep_labels.start()


def solve_and_pack(level, levels, at, copies):
    solved, live = at["solved"], at["live"]
    slots = solved.shape[0]
    last = level == levels - 1
    left = levels - level
    rhs = at["rhs"].at[level]
    totals = [at[name] for name in chains(level)]

    def total_of(part):
        return sum((total[part] for total in totals[1:]), totals[0][part])

    solve(live[level], lambda slot: rhs[slot] - total_of(slot), at["diag"].at[level], solved)
    if last:
        wait(copies.start(solved, at["answer"].at[level]))
    else:
        off = at["off"].at[level]
        values = products(lambda i: solved[at["source"][level, i]], off, 0, off.shape[0])
        for record, value in enumerate(values):
            at["outgoing"][at["place"][level, record]] = value
        at["after"][...] = total_of(slice(slots, left * slots))


def later_kernel(level, levels, owners, names, *refs):
    at = dict(zip(names, refs))
    copies = Copies(at.get("sems"))
    live = at["live"]
    ahead = []
    if level == levels - 1:
        ahead = [copies.start(at[f"solved_{before}"], at["answer"].at[before]) for before in range(level)]

    keep_labels = copies.make(at["turned"], at["labels"]) if level == 1 else None

    def region(work):
        if level == 1 or level == levels - 1:
            pl.when(live[level] >= 0)(work)
        else:
            work()

    def add():
        add_arrived(level, levels, owners, at, keep_labels)
        if level > 1:
            solve_and_pack(level, levels, at, copies)

    region(add)
    if level == 1:
        region(lambda: solve_and_pack(level, levels, at, copies))

    wait(*ahead, *([keep_labels] if level == 1 else []))


def shards(right_side, diag_inverse, off_blocks, live_counts, source_slot, target_owner, target_block):
    levels, slots, rows, width = right_side.shape
    records = off_blocks.shape[1]
    owners = lax.axis_size(AXES)
    steps = levels - 1
    chunk = CAP * rows
    f32, bf16, i32 = jnp.float32, jnp.bfloat16, jnp.int32
    near, table, semaphores = pltpu.VMEM, pltpu.SMEM, pltpu.SemaphoreType.DMA
    rows_shape = (slots, rows, width)
    diag_shape, off_shape = (slots, width, width), (records, width, width)
    arguments = (live_counts.reshape(levels), source_slot, target_owner, target_block)
    arguments += (right_side, diag_inverse, off_blocks)
    arguments = [pltpu.with_memory_space_constraint(x, pltpu.HBM) for x in arguments]
    rhs, diag, off = (
        pltpu.with_memory_space_constraint(x, pltpu.VMEM) for x in (right_side, diag_inverse, off_blocks)
    )

    def exchange(parts):
        return lax.all_to_all(parts, AXES, split_axis=0, concat_axis=0, tiled=True)

    outgoing, solved, live, source, place = pl.pallas_call(
        functools.partial(first_kernel, owners),
        out_shape=[
            near((owners * (chunk + 1), 1, width), f32),
            near(rows_shape, f32),
            table((levels,), i32),
            table((steps, records), i32),
            table((steps, records), i32),
        ],
        in_specs=[HBM] * 7,
        out_specs=[VMEM, VMEM, SMEM, SMEM, SMEM],
        scratch_shapes=[
            near((steps, records), i32),
            near((steps, records), i32),
            near((steps, records), i32),
            near(rows_shape, f32),
            near(diag_shape, bf16),
            near(off_shape, bf16),
            semaphores((7,)),
        ],
        name="level_0",
        compiler_params=PARAMS,
    )(*arguments)
    arrived = exchange(outgoing.reshape(owners, chunk + 1, 1, width)).reshape(owners * (chunk + 1), 1, width)

    solved = [solved]
    labels = before = None
    for level in range(1, levels):
        last = level == levels - 1
        left = levels - level
        ins = [("live", live, SMEM), ("rhs", rhs, VMEM), ("diag", diag, VMEM), ("arrived", arrived, VMEM)]
        outs = []
        scratch = [(name, near((left * slots + 1, rows, width), f32)) for name in chains(level)]
        if level == 1 or last:
            scratch.append(("sems", semaphores((levels if last else 1,))))
        if level == 1:
            outs.append(("labels", table((steps * CAP, owners), i32), SMEM))
            scratch += [("gathered", near((owners, width), f32)), ("turned", near((steps * CAP, owners), i32))]
        else:
            ins += [("labels", labels, SMEM), ("before", before, VMEM)]
        if last:
            ins += [(f"solved_{before}", value, VMEM) for before, value in enumerate(solved)]
            outs.append(("answer", pltpu.HBM((levels, *rows_shape), f32), HBM))
            scratch.append(("solved", near(rows_shape, f32)))
        else:
            ins += [("source", source, SMEM), ("place", place, SMEM), ("off", off, VMEM)]
            outs.append(("solved", near(rows_shape, f32), VMEM))
            outs.append(("outgoing", near((owners * CAP, rows, width), f32), VMEM))
            outs.append(("after", near(((left - 1) * slots, rows, width), f32), VMEM))
        names = [name for name, *_ in ins + outs + scratch]
        made = pl.pallas_call(
            functools.partial(later_kernel, level, levels, owners, names),
            out_shape=[shape for _, shape, _ in outs],
            in_specs=[spec for *_, spec in ins],
            out_specs=[spec for *_, spec in outs],
            scratch_shapes=[shape for _, shape in scratch],
            name=f"level_{level}",
            compiler_params=PARAMS,
        )(*[value for _, value, _ in ins])
        made = dict(zip([name for name, *_ in outs], made))
        if last:
            return made["answer"]
        solved.append(made["solved"])
        before = made["after"]
        labels = made.get("labels", labels)
        arrived = exchange(made["outgoing"].reshape(owners, chunk, width)).reshape(owners * CAP, rows, width)


def solution(mesh):
    spread = P(None, AXES)
    return jax.shard_map(
        shards,
        mesh=mesh,
        in_specs=(P(None, AXES, None, None),) * 3 + (spread,) * 4,
        out_specs=P(None, AXES, None, None),
        check_vma=False,
    )
```
